32 devices in a mesh: role: 4 (over z), dp: 2 (over x), tp: 4 (over y, core).
Axes of the slice: x: 2, y: 2, z: 4, core: 2. Of those that a mesh axis runs over, the one named last changes fastest.
Arguments:
- activations: bfloat16 [2048, 8192], P(('role', 'dp'), 'tp'), may hold values from -6 to 6
- cotangent: bfloat16 [2048, 14336], P(('role', 'dp'), 'tp'), may hold values from -6 to 6
- block_keep: int32 [8], P(('role', 'dp')), may hold values 0 or 1
- input_factor: float32 [64, 8192], P(('role', 'dp'), 'tp'), may hold values from -0.5 to 0.5
- input_mean: float32 [64, 8192], P(('role', 'dp'), 'tp'), may hold values from -6 to 6
- input_square: float32 [64, 8192], P(('role', 'dp'), 'tp'), may hold values from 0.5 to 4
- output_factor: float32 [64, 14336], P(('role', 'dp'), 'tp'), may hold values from -0.3125 to 0.3125
- output_mean: float32 [64, 14336], P(('role', 'dp'), 'tp'), may hold values from -6 to 6
- output_square: float32 [64, 14336], P(('role', 'dp'), 'tp'), may hold values from 0.5 to 4
- frozen_base_rows: bfloat16 [14336, 8192], P(('dp', 'tp')), may hold values from -0.0625 to 0.0625
- prompts: bfloat16 [1024, 8192], P(('role', 'dp', 'tp')), may hold values from -6 to 6
Outputs:
- updated_input: float32 [64, 8192], P(('role', 'dp'), 'tp')
- updated_output: float32 [64, 14336], P(('role', 'dp'), 'tp')
- mean_input: float32 [64, 8192], P(('role', 'dp'), 'tp')
- mean_output: float32 [64, 14336], P(('role', 'dp'), 'tp')
- square_input: float32 [64, 8192], P(('role', 'dp'), 'tp')
- square_output: float32 [64, 14336], P(('role', 'dp'), 'tp')
- merged_weight_rows: bfloat16 [14336, 8192], P(('dp', 'tp'))
- projected: bfloat16 [14336, 1024], P(('dp', 'tp'), 'role')
The draws below stay inside these ranges and needn't reach their ends.
All inputs are finite; a program needn't handle non-finite values. No bound on the sum of `block_keep` on one device may be relied on, other than what follows from the above.
Results may differ from the reference program's by a relative error of at most 0.006.
Values may be sent and summed in bfloat16 or wider, within the bound.
No kernel may reach another device: no remote copies, remote signals or barrier semaphores. Data moves between devices by JAX's collectives and lax.ppermute only.
A program may use at most 128 MiB of HBM per device.

```python
import math
import jax
import jax.numpy as jnp
from jax import lax

D = 8192
FFW = 14336
RANK = 64
ROLLOUT_TOKENS = 256
TOKENS = 2048
BLOCKS = 8
PROMPTS = 1024


def touch_ends(result, key, low, high):
    dims = result.shape
    place = [jax.random.randint(jax.random.fold_in(key, axis), (), 0, dims[axis]) for axis in range(len(dims))]
    result = result.at[tuple(place)].set(low)
    longest = dims.index(max(dims))
    place[longest] = (place[longest] + 1) % dims[longest]
    return result.at[tuple(place)].set(high)


def shard_levels(own_key, shape, cuts, smallest, top_value):
    factor_of, own = 1.0, jax.random.fold_in(own_key, 6)
    for dim, shards_of in cuts:
        draws = jnp.exp(jax.random.uniform(jax.random.fold_in(own, dim), (shards_of,), jnp.float32, smallest / len(cuts), top_value / len(cuts)))
        factor_of = factor_of * jnp.repeat(draws, shape[dim] // shards_of).reshape([-1 if axis == dim else 1 for axis in range(len(shape))])
    return factor_of


def scatter_about(own_key, shape, spread, limit, shards=(), dtype=jnp.bfloat16):
    array = jax.random.normal(own_key, shape, jnp.float32) * spread
    if len(shards) > 0:
        array = shard_levels(own_key, shape, shards, -0.22, 0.18) * array
    return jnp.clip(array, min=-limit, max=limit).astype(dtype)


def setup_inputs(seed: int = 0) -> dict:
    key_of = jax.random.split(jax.random.key(seed), 12)
    return {
        "activations": scatter_about(key_of[0], (TOKENS, D), 1.0, 6.0, ((0, 8), (1, 4))),
        "cotangent": scatter_about(key_of[1], (TOKENS, FFW), 1.0, 6.0, ((0, 8), (1, 4))),
        "block_keep": touch_ends((jax.random.randint(key_of[2], (BLOCKS,), 0, 4) < 3).astype(jnp.int32), jax.random.fold_in(key_of[2], 1), 0, 1),
        "input_factor": scatter_about(key_of[3], (RANK, D), 0.035, 0.5, ((0, 8), (1, 4)), jnp.float32),
        "input_mean": scatter_about(key_of[4], (RANK, D), 1.0, 6.0, ((0, 8), (1, 4)), jnp.float32),
        "input_square": jnp.clip(jnp.exp(math.log(4.0) - 2.0794415 * jax.random.uniform(key_of[5], (RANK, D), jnp.float32) ** shard_levels(key_of[5], (RANK, D), ((0, 8), (1, 4)), -0.2, 0.2)), 0.5, 4.0),
        "output_factor": scatter_about(key_of[6], (RANK, FFW), 0.02, 0.3125, ((0, 8), (1, 4)), jnp.float32),
        "output_mean": scatter_about(key_of[7], (RANK, FFW), 1.0, 6.0, ((0, 8), (1, 4)), jnp.float32),
        "output_square": jnp.clip(jnp.exp(math.log(4.0) - 2.0794415 * jax.random.uniform(key_of[8], (RANK, FFW), jnp.float32) ** shard_levels(key_of[8], (RANK, FFW), ((0, 8), (1, 4)), -0.2, 0.2)), 0.5, 4.0),
        "frozen_base_rows": scatter_about(key_of[9], (FFW, D), D ** -0.5, 0.0625, ((0, 8),)),
        "prompts": scatter_about(key_of[10], (PROMPTS, D), 1.0, 6.0, ((0, 32),)),
    }


adapter_scale = 2.0
learn_rate = 0.004
beta_one = 0.9
beta_two = 0.95
epsilon = 1e-08
first_fix = 1.0 - 0.9 ** 20
second_fix = 1.0 - 0.95 ** 20

def adam_update(factor, moment, square, gradient):
    moment_new = beta_one * moment + (1.0 - beta_one) * gradient
    square_new = beta_two * square + (1.0 - beta_two) * gradient * gradient
    factor_new = factor - learn_rate * (moment_new / first_fix) / (jnp.sqrt(square_new / second_fix) + epsilon)
    return (factor_new, moment_new, square_new)

def masked(values, block_keep):
    blocks = block_keep.shape[0]
    reshaped_rows = values.reshape(blocks, values.shape[0] // blocks, values.shape[1])
    weighted = reshaped_rows * block_keep.astype(jnp.float32)[:, None, None]
    return weighted.reshape(values.shape).astype(jnp.bfloat16)

def contract_rows(left, right):
    return lax.dot_general(left, right, (((0,), (0,)), ((), ())), preferred_element_type=jnp.float32)

def contract_cols(left, right):
    return lax.dot_general(left, right, (((1,), (1,)), ((), ())), preferred_element_type=jnp.float32)

def reference(activations, cotangent, block_keep, input_factor, input_mean, input_square, output_factor, output_mean, output_square, frozen_base_rows, prompts):
    input_rows = input_factor.astype(jnp.bfloat16)
    output_rows = output_factor.astype(jnp.bfloat16)
    low_input = jnp.dot(activations, input_rows.T, preferred_element_type=jnp.float32)
    low_grad = jnp.dot(cotangent, output_rows.T, preferred_element_type=jnp.float32)
    input_kept = masked(low_input, block_keep)
    grad_kept = masked(low_grad, block_keep)
    adapter_factor_scale = adapter_scale / ROLLOUT_TOKENS
    input_grad = contract_rows(grad_kept, activations) * adapter_factor_scale
    output_grad = contract_rows(input_kept, cotangent) * adapter_factor_scale
    input_new, input_moment, input_second = adam_update(input_factor, input_mean, input_square, input_grad)
    output_new, output_moment, output_second = adam_update(output_factor, output_mean, output_square, output_grad)
    adapter_delta_rows = contract_rows(output_new.astype(jnp.bfloat16), input_new.astype(jnp.bfloat16))
    merged_weight_rows = (frozen_base_rows.astype(jnp.float32) + adapter_scale * adapter_delta_rows).astype(jnp.bfloat16)
    projected = contract_cols(merged_weight_rows, prompts).astype(jnp.bfloat16)
    return (input_new, output_new, input_moment, output_moment, input_second, output_second, merged_weight_rows, projected)
```

```python
import functools

import jax
import jax.numpy as jnp
from jax import lax
from jax.experimental import pallas as pl
from jax.experimental.pallas import tpu as pltpu
from jax.sharding import PartitionSpec as P

ROLLOUT_TOKENS = 256

adapter_scale = 2.0
learn_rate = 0.004
beta_one = 0.9
beta_two = 0.95
epsilon = 1e-08
first_fix = 1.0 - 0.9**20
second_fix = 1.0 - 0.95**20

F32 = jnp.float32
BF16 = jnp.bfloat16
VMEM = pltpu.VMEM
MIB = 1024 * 1024


def adam_update(factor, moment, square, gradient):
    moment_new = beta_one * moment + (1.0 - beta_one) * gradient
    square_new = beta_two * square + (1.0 - beta_two) * gradient * gradient
    factor_new = factor - learn_rate * (moment_new / first_fix) / (
        jnp.sqrt(square_new / second_fix) + epsilon
    )
    return (factor_new, moment_new, square_new)


def contract_rows(left, right):
    return lax.dot_general(
        left, right, (((0,), (0,)), ((), ())), preferred_element_type=F32
    )


def contract_cols(left, right):
    return lax.dot_general(
        left, right, (((1,), (1,)), ((), ())), preferred_element_type=F32
    )


def masked(values, block_keep):
    blocks = block_keep.shape[0]
    reshaped_rows = values.reshape(blocks, values.shape[0] // blocks, values.shape[1])
    weighted = reshaped_rows * block_keep.astype(F32)[:, None, None]
    return weighted.reshape(values.shape).astype(BF16)


def plain_body(
    activations,
    cotangent,
    block_keep,
    input_factor,
    input_mean,
    input_square,
    output_factor,
    output_mean,
    output_square,
    frozen_base_rows,
    prompts,
):
    input_rows, output_rows = (
        lax.all_gather(input_factor.astype(BF16), ("role", "dp"), axis=0, tiled=True),
        lax.all_gather(output_factor.astype(BF16), ("role", "dp"), axis=0, tiled=True),
    )
    low_input = jnp.dot(activations, input_rows.T, preferred_element_type=F32)
    low_grad = jnp.dot(cotangent, output_rows.T, preferred_element_type=F32)
    low_input, low_grad = lax.psum((low_input, low_grad), "tp")
    input_kept = masked(low_input, block_keep)
    grad_kept = masked(low_grad, block_keep)
    input_part = contract_rows(grad_kept, activations)
    output_part = contract_rows(input_kept, cotangent)
    group_input, group_output = (
        lax.psum_scatter(input_part, "role", scatter_dimension=0, tiled=True),
        lax.psum_scatter(output_part, "role", scatter_dimension=0, tiled=True),
    )
    input_sum, output_sum = (
        lax.psum_scatter(group_input, "dp", scatter_dimension=0, tiled=True),
        lax.psum_scatter(group_output, "dp", scatter_dimension=0, tiled=True),
    )
    factor_scale = adapter_scale / ROLLOUT_TOKENS
    input_new, input_moment, input_second = adam_update(
        input_factor, input_mean, input_square, input_sum * factor_scale
    )
    output_new, output_moment, output_second = adam_update(
        output_factor, output_mean, output_square, output_sum * factor_scale
    )
    input_cols, output_cols = (
        lax.all_gather(input_new.astype(BF16), ("role", "dp"), axis=0, tiled=True),
        lax.all_gather(output_new.astype(BF16), ("role", "dp"), axis=0, tiled=True),
    )
    input_whole, output_whole = (
        lax.all_gather(input_cols, "tp", axis=1, tiled=True),
        lax.all_gather(output_cols, "tp", axis=1, tiled=True),
    )
    rows_here = frozen_base_rows.shape[0]
    row_block = lax.axis_index("dp") * lax.axis_size("tp") + lax.axis_index("tp")
    output_slice = lax.dynamic_slice_in_dim(
        output_whole, row_block * rows_here, rows_here, 1
    )
    adapter_delta_rows = contract_rows(output_slice, input_whole)
    merged_weight_rows = (
        frozen_base_rows.astype(F32) + adapter_scale * adapter_delta_rows
    ).astype(BF16)
    group_prompts = lax.all_gather(prompts, ("dp", "tp"), axis=0, tiled=True)
    projected = contract_cols(merged_weight_rows, group_prompts)
    return (
        input_new,
        output_new,
        input_moment,
        output_moment,
        input_second,
        output_second,
        merged_weight_rows,
        projected.astype(BF16),
    )


def swap(value, axis, size, step):
    return lax.ppermute(value, axis, [(i, i ^ step) for i in range(size)])


def params(mib):
    return pltpu.CompilerParams(vmem_limit_bytes=mib * MIB)


def cost(flops, nbytes):
    return pl.CostEstimate(flops=flops, bytes_accessed=nbytes, transcendentals=0)


def whole():
    return pl.BlockSpec(memory_space=VMEM)


def low_kernel(count, width, *refs):
    pieces, (act, cot, out) = refs[:count], refs[count:]
    rank = out.shape[0] // 2
    left = jnp.concatenate([p[:, :width].astype(F32) for p in pieces], 0).astype(BF16)
    right = jnp.concatenate([p[:, width:].astype(F32) for p in pieces], 0).astype(BF16)
    out[:rank] = contract_cols(left, act[...])
    out[rank:] = contract_cols(right, cot[...])


def grad_kernel(count, width, keep, *refs):
    parts = refs[: len(refs) - 2 - count]
    act, cot = refs[len(parts) : len(parts) + 2]
    outs = refs[len(parts) + 2 :]
    low = parts[0][...]
    for part in parts[1:]:
        low = low + part[...]
    kept = (low * keep[0].astype(F32)).astype(BF16)
    rank = kept.shape[0] // 2
    rows = rank // count
    input_part = jnp.dot(kept[rank:], act[...], preferred_element_type=F32)
    output_part = jnp.dot(kept[:rank], cot[...], preferred_element_type=F32)
    for k, out in enumerate(outs):
        span = slice(k * rows, (k + 1) * rows)
        out[:, :width] = input_part[span].astype(out.dtype)
        out[:, width:] = output_part[span].astype(out.dtype)


def adam_kernel(count, width, place, *refs):
    parts = refs[:count]
    fa, ma, va, fb, mb, vb = refs[count : count + 6]
    nfa, nfb, nma, nmb, nva, nvb, send_a = refs[count + 6 : count + 13]
    send_b, hold = refs[count + 13 : -1], refs[-1]
    total = parts[0][...]
    for part in parts[1:]:
        total = total + part[...].astype(F32)
    total = total * (adapter_scale / ROLLOUT_TOKENS)
    nfa[...], nma[...], nva[...] = adam_update(
        fa[...], ma[...], va[...], total[:, :width]
    )
    nfb[...], nmb[...], nvb[...] = adam_update(
        fb[...], mb[...], vb[...], total[:, width:]
    )
    send_a[...] = nfa[...].astype(BF16)
    hold[...] = nfb[...]
    wide = send_b[0].shape[1]
    for k, out in enumerate(send_b):
        start = pl.multiple_of((place[0] ^ k) * wide, 128)
        out[...] = hold[:, pl.ds(start, wide)].astype(BF16)


def join_kernel(width, *refs):
    pieces, (out_a, out_b) = refs[:-2], refs[-2:]
    whole_rows = jnp.concatenate([p[...].astype(F32) for p in pieces], 0).astype(BF16)
    out_a[...] = whole_rows[:, :width]
    out_b[...] = whole_rows[:, width:]


def early_kernel(count, place, *refs):
    pieces, (base, early, wide, sem) = refs[:count], refs[count:]

    @pl.when(pl.program_id(0) == 0)
    def _():
        rows = pieces[0].shape[0]
        copies = []
        for k, piece in enumerate(pieces):
            start = pl.multiple_of(place[k] * rows, rows)
            copies.append(
                pltpu.make_async_copy(piece, wide.at[pl.ds(start, rows)], sem.at[k])
            )
        for copy in copies:
            copy.start()
        for copy in copies:
            copy.wait()

    early[...] = contract_cols(base[...], wide[...])


def merge_kernel(first, last, slot, *refs):
    refs = list(refs)
    a, b, base, wide = refs[:4]
    rest = refs[4:]
    if not first:
        rest = rest[1:]
        seen, rest = rest[0], rest[1:]
    if last:
        early, rest = rest[0], rest[1:]
    merged, low = rest[0], rest[1]
    here = contract_cols(a[...], wide[...])

    @pl.when(pl.program_id(0) == 0)
    def _():
        low[...] = here if first else here + seen[...]

    delta = contract_rows(b[...], a[...])
    merged[...] = (base[...].astype(F32) + adapter_scale * delta).astype(BF16)
    if last:
        full = low[...]
        high = full.astype(BF16)
        rest_low = (full - high.astype(F32)).astype(BF16)
        twice = jnp.concatenate([b[...], b[...]], 0)
        both = jnp.concatenate([high, rest_low], 0)
        rest[2][...] = (early[...] + adapter_scale * contract_rows(twice, both)).astype(
            BF16
        )


def exchange_body(
    sizes,
    activations,
    cotangent,
    block_keep,
    input_factor,
    input_mean,
    input_square,
    output_factor,
    output_mean,
    output_square,
    frozen_base_rows,
    prompts,
):
    roles, dps, tps = sizes
    both = ("role", "dp")
    owners = roles * dps
    tokens, width = activations.shape
    hidden = cotangent.shape[1]
    rows = input_factor.shape[0]
    rank = rows * owners
    base_rows, model = frozen_base_rows.shape
    asked = prompts.shape[0]
    d, t = lax.axis_index("dp"), lax.axis_index("tp")
    struct = jax.ShapeDtypeStruct

    mine = jnp.concatenate([input_factor.astype(BF16), output_factor.astype(BF16)], 1)
    pieces = [mine] + [swap(mine, both, owners, k) for k in range(1, owners)]
    low = pl.pallas_call(
        functools.partial(low_kernel, owners, width),
        out_shape=struct((2 * rank, tokens), F32),
        in_specs=[whole()] * (owners + 2),
        out_specs=whole(),
        compiler_params=params(24),
        cost_estimate=cost(2 * rank * tokens * (width + hidden), 4 * MIB),
        name="low",
    )(*pieces, activations, cotangent)
    lows = [low] + [swap(low, "tp", tps, k) for k in range(1, tps)]

    grads = pl.pallas_call(
        functools.partial(grad_kernel, owners, width),
        out_shape=[struct((rows, width + hidden), F32)]
        + [struct((rows, width + hidden), BF16)] * (owners - 1),
        in_specs=[pl.BlockSpec(memory_space=pltpu.SMEM)] + [whole()] * (tps + 2),
        out_specs=[whole()] * owners,
        compiler_params=params(24),
        cost_estimate=cost(2 * rank * tokens * (width + hidden), 4 * MIB),
        name="grad",
    )(block_keep, *lows, activations, cotangent)
    parts = [grads[0]] + [
        swap(grads[k], both, owners, k) for k in range(1, owners)
    ]

    share = hidden // dps
    small_a, small_b = struct((rows, width), F32), struct((rows, hidden), F32)
    adam = pl.pallas_call(
        functools.partial(adam_kernel, owners, width),
        out_shape=[small_a, small_b] * 3
        + [struct((rows, width), BF16)]
        + [struct((rows, share), BF16)] * dps,
        in_specs=[pl.BlockSpec(memory_space=pltpu.SMEM)] + [whole()] * (owners + 6),
        out_specs=[whole()] * (7 + dps),
        scratch_shapes=[VMEM((rows, hidden), F32)],
        compiler_params=params(16),
        cost_estimate=cost(40 * rows * (width + hidden), 4 * MIB),
        name="adam",
    )(
        d[None],
        *parts,
        input_factor,
        input_mean,
        input_square,
        output_factor,
        output_mean,
        output_square,
    )
    outs, send_a, send_b = adam[:6], adam[6], adam[7:]

    near_a = [send_a] + [swap(send_a, "dp", dps, k) for k in range(1, dps)]
    near_b = [
        lax.ppermute(
            send_b[k],
            ("dp", "tp"),
            [
                (i, (i % tps) * dps + ((i // tps) ^ k))
                for i in range(dps * tps)
            ],
        )
        for k in range(dps)
    ]
    turn = d ^ ((d * tps + t) % dps)
    stacked = jnp.stack(near_b, 0)
    ordered = [
        lax.dynamic_index_in_dim(stacked, turn ^ k, 0, keepdims=False)
        for k in range(dps)
    ]
    plane = jnp.concatenate(
        [jnp.concatenate([near_a[k], ordered[k]], 1) for k in range(dps)], 0
    )
    planes = [plane] + [swap(plane, "role", roles, k) for k in range(1, roles)]
    a_own, b_here = pl.pallas_call(
        functools.partial(join_kernel, width),
        out_shape=[struct((rank, width), BF16), struct((rank, share), BF16)],
        in_specs=[whole()] * roles,
        out_specs=[whole()] * 2,
        compiler_params=params(8),
        cost_estimate=cost(rank * width, MIB),
        name="join",
    )(*planes)
    slots = {0: a_own}
    step = 1
    while step < tps:
        step *= 2
    held = [0]
    step //= 2
    order = [0]
    reach = []
    k = 1
    while k < tps:
        reach.append(k)
        k *= 2
    for k in range(1, tps):
        top = max(bit for bit in reach if k & bit)
        low_part = k ^ top
        if low_part:
            slots[k] = swap(slots[top], "tp", tps, low_part)
        else:
            slots[k] = swap(a_own, "tp", tps, top)

    asks = {(0, 0): prompts}
    for kd in range(1, dps):
        asks[kd, 0] = swap(prompts, "dp", dps, kd)
    for kd in range(dps):
        for k in reversed(reach):
            for kt in [kt for (od, kt) in list(asks) if od == kd]:
                asks[kd, kt ^ k] = swap(asks[kd, kt], "tp", tps, k)
    keys = sorted(asks)
    spots = jnp.stack([(d ^ kd) * tps + (t ^ kt) for kd, kt in keys])
    gathered = asked * len(keys)
    tile = 256 if base_rows % 256 == 0 else base_rows
    early, wide = pl.pallas_call(
        functools.partial(early_kernel, len(keys)),
        out_shape=[struct((base_rows, gathered), F32), struct((gathered, model), BF16)],
        grid=(base_rows // tile,),
        in_specs=[pl.BlockSpec(memory_space=pltpu.SMEM)]
        + [pl.BlockSpec(memory_space=pl.ANY)] * len(keys)
        + [pl.BlockSpec((tile, model), lambda i: (i, 0))],
        out_specs=[
            pl.BlockSpec((tile, gathered), lambda i: (i, 0)),
            pl.BlockSpec((gathered, model), lambda i: (0, 0)),
        ],
        scratch_shapes=[pltpu.SemaphoreType.DMA((len(keys),))],
        compiler_params=params(40),
        cost_estimate=cost(
            2 * base_rows * gathered * model, 2 * (base_rows + 2 * gathered) * model
        ),
        name="early",
    )(spots, *[asks[key] for key in keys], frozen_base_rows)

    merged = low_sum = None
    for k in range(tps):
        first, last = k == 0, k == tps - 1
        args = [slots[k], b_here, frozen_base_rows, wide]
        specs = [
            pl.BlockSpec((rank, width), lambda i, s: (0, 0)),
            pl.BlockSpec((rank, tile), lambda i, s: (0, i)),
            pl.BlockSpec((tile, width), lambda i, s: (i, s[0])),
            pl.BlockSpec((gathered, width), lambda i, s: (0, s[0])),
        ]
        alias = {}
        out_shape = [
            struct((base_rows, model), BF16),
            struct((rank, gathered), F32),
        ]
        out_specs = [
            pl.BlockSpec((tile, width), lambda i, s: (i, s[0])),
            pl.BlockSpec((rank, gathered), lambda i, s: (0, 0)),
        ]
        if not first:
            args += [merged, low_sum]
            specs += [
                pl.BlockSpec(memory_space=pl.ANY),
                pl.BlockSpec((rank, gathered), lambda i, s: (0, 0)),
            ]
            alias = {5: 0}
        if last:
            args.append(early)
            specs.append(pl.BlockSpec((tile, gathered), lambda i, s: (i, 0)))
            out_shape.append(struct((base_rows, gathered), BF16))
            out_specs.append(pl.BlockSpec((tile, gathered), lambda i, s: (i, 0)))
        results = pl.pallas_call(
            functools.partial(merge_kernel, first, last),
            out_shape=out_shape,
            grid_spec=pltpu.PrefetchScalarGridSpec(
                num_scalar_prefetch=1,
                grid=(base_rows // tile,),
                in_specs=specs,
                out_specs=out_specs,
            ),
            input_output_aliases=alias,
            compiler_params=params(24),
            cost_estimate=cost(
                2 * base_rows * rank * width, 4 * base_rows * width
            ),
            name=f"merge{k}",
        )((t ^ k)[None], *args)
        merged, low_sum = results[0], results[1]
    projected = results[2]
    return (*outs, merged, projected)


def power_of_two(n):
    return n & (n - 1) == 0


def solution(mesh):
    roles, dps, tps = (mesh.shape[name] for name in ("role", "dp", "tp"))
    small = roles * dps <= 8 and 1 < tps <= 8 and tps % dps == 0
    if small and all(power_of_two(n) for n in (roles, dps, tps)):
        body = functools.partial(exchange_body, (roles, dps, tps))
    else:
        body = plain_body
    owned = P(("role", "dp"), "tp")
    return jax.shard_map(
        body,
        mesh=mesh,
        in_specs=(
            owned,
            owned,
            P(("role", "dp")),
            *[owned] * 6,
            P(("dp", "tp"), None),
            P(("role", "dp", "tp"), None),
        ),
        out_specs=(
            *[owned] * 6,
            P(("dp", "tp"), None),
            P(("dp", "tp"), "role"),
        ),
        check_vma=False,
    )
```
